32 devices in a mesh: src: 4 (over y, x), col: 8 (over z, core).
Axes of the slice: x: 2, y: 2, z: 4, core: 2. Of those that a mesh axis runs over, the one named last changes fastest.
Arguments:
- saved_tables: float32 [4, 16384, 256], P('src', 'col'), may hold values from -6 to 6
- saved_state: float32 [4, 16384], P('src', 'col'), may hold values from 0.05 to 4
- slot_table: int32 [4], replicated, may hold values from 0 to 3, each once
- row_ids: int32 [4, 2048], replicated, may hold values from 0 to 16383
- grads: float32 [4, 256, 2048], P('src', 'col'), may hold values from -6 to 6
Outputs:
- tables_out: float32 [4, 256, 16384], P('src', 'col')
- state_out: float32 [4, 16384], P('src')
The draws below stay inside these ranges and needn't reach their ends.
Inputs may be any that keep to these rules, and one draw needn't show every extreme that they name: `slot_table`: each table is in exactly one slot. `row_ids`: row ids may repeat.
All inputs are finite; a program needn't handle non-finite values.
Results may differ from the reference program's by a relative error of at most 0.00002.
Values sent between devices are 32-bit elements; how exact they have to be, the bound alone decides.
A program may use at most 192 MiB of HBM per device.

```python
import math
import jax
import jax.numpy as jnp
import numpy as np
from jax import lax

D = 256
UPD = 2048
NT = 4
ROWS = 16384


def plant(drawn, rng, smallest, top_value):
    place = [jax.random.randint(jax.random.fold_in(rng, axis), (), 0, length) for axis, length in enumerate(drawn.shape)]
    main_axis = drawn.shape.index(max(drawn.shape))
    beside = place[:main_axis] + [(place[main_axis] + 1) % drawn.shape[main_axis]] + place[main_axis + 1:]
    return drawn.at[tuple(place)].set(smallest).at[tuple(beside)].set(top_value)


def levels(own_key, shape, split, least, top_value):
    gain, own = 1.0, jax.random.fold_in(own_key, 6)
    for dim, parts in split:
        steps = jnp.exp(jax.random.uniform(jax.random.fold_in(own, dim), (parts,), jnp.float32, least / len(split), top_value / len(split)))
        gain = gain * jnp.repeat(steps, shape[dim] // parts).reshape([-1 if axis == dim else 1 for axis in range(len(shape))])
    return gain


def cumulative_ranks(number_of, lean):
    weights = [(1 << 20) // math.isqrt(standing ** lean) + 1 for standing in range(1, number_of + 1)]
    deviation = 1 + sum(weights) // (1 << 30)
    return np.cumsum(np.array([max(1, weight // deviation) for weight in weights]))


def ranked_ids(stream_key, extent, count, slope):
    grid = cumulative_ranks(count, slope)
    ticket = jax.random.randint(jax.random.fold_in(stream_key, 1), extent, 0, int(grid[count - 1]))
    grade = jnp.searchsorted(jnp.asarray(grid, jnp.int32), ticket, side="right")
    return jax.random.permutation(jax.random.fold_in(stream_key, 2), count)[grade].astype(jnp.int32)


def gaussian(stream_key, dims, scale, reach, shards=(), held_as=jnp.bfloat16):
    factor_of = levels(stream_key, dims, shards, -0.22, 0.18) if shards else 1.0
    values = jax.random.normal(stream_key, dims, jnp.float32) * scale * factor_of
    return jnp.minimum(jnp.maximum(values, -reach), reach).astype(held_as)


def setup_inputs(seed: int = 0) -> dict:
    streams_of = jax.random.split(jax.random.key(seed), 6)
    saved_tables = gaussian(streams_of[0], (NT, ROWS, D), 1.0, 6.0, ((0, 4), (1, 8)), jnp.float32)
    saved_state = jnp.clip(jnp.exp(math.log(4.0) - 4.3820266 * jax.random.uniform(streams_of[1], (NT, ROWS), jnp.float32) ** levels(streams_of[1], (NT, ROWS), ((0, 4), (1, 8)), -0.2, 0.2)), 0.05, 4.0)
    slot_table = jax.random.permutation(streams_of[2], NT).astype(jnp.int32)
    row_ids = plant(ranked_ids(streams_of[3], (NT, UPD), ROWS, 2), jax.random.fold_in(streams_of[3], 3), 0, ROWS - 1).astype(jnp.int32)
    grads = gaussian(streams_of[4], (NT, D, UPD), 1.0, 6.0, ((0, 4), (1, 8)), jnp.float32)
    return {"saved_tables": saved_tables, "saved_state": saved_state, "slot_table": slot_table, "row_ids": row_ids, "grads": grads}


learn_rate = 0.5
epsilon = 1e-08

def reference(saved_tables, saved_state, slot_table, row_ids, grads):

    def one_slot(slot):
        table = slot_table[slot]
        weights = saved_tables[slot]
        state = saved_state[slot]
        summed = jnp.zeros((ROWS, D), jnp.float32).at[row_ids[table]].add(grads[table].T)
        new_state = state + lax.optimization_barrier(jnp.sum(summed * summed, axis=1)) / D
        new_weights = weights - learn_rate * summed / (jnp.sqrt(new_state)[:, None] + epsilon)
        return (new_weights.T, new_state)
    result = lax.map(one_slot, jnp.arange(NT, dtype=jnp.int32))
    return (result[0], result[1])
```

```python
import functools

import jax
import jax.numpy as jnp
from jax import lax
from jax.experimental import pallas as pl
from jax.experimental.pallas import tpu as pltpu
from jax.sharding import PartitionSpec as P

learn_rate = 0.5
epsilon = 1e-08

MESH = pl.DeviceIdType.MESH
LANES = 128
LOW = 256
GROUP = 4
CHUNKS = 4


def kernel(ns, nc, tab, state, slot_table, ids, grads, out, state_out,
           x, xt, tb, summed, gbuf, parts, hib, onehot, sq, rs, stbuf,
           x_sem, g_sem, gs_send, gs_recv, t_send, t_recv,
           q_send, q_recv, s_send, s_recv, o_sem):
    k = lax.axis_index("src")
    d = lax.axis_index("col")
    rows, width = x.shape
    cols, upd = gbuf.shape[1], gbuf.shape[2]
    total_rows = tb.shape[1]
    per = LANES // cols
    ch = rows // CHUNKS

    loads = []
    for c in range(CHUNKS):
        span = pl.ds(c * ch, ch)
        load = pltpu.make_async_copy(tab.at[0, span], x.at[span], x_sem.at[c])
        load.start()
        loads.append(load)
    own_grad = pltpu.make_async_copy(grads.at[0], gbuf.at[k], g_sem)
    own_grad.start()

    barrier = pltpu.get_barrier_semaphore()
    for m in range(1, nc):
        pl.semaphore_signal(barrier, inc=1, device_id=(k, d ^ m), device_id_type=MESH)
    for m in range(1, ns):
        pl.semaphore_signal(barrier, inc=1, device_id=(k ^ m, d), device_id_type=MESH)
    pl.semaphore_wait(barrier, nc + ns - 2)

    def grad_copy(m, owner):
        return pltpu.make_async_remote_copy(
            src_ref=grads.at[0], dst_ref=gbuf.at[owner],
            send_sem=gs_send.at[m], recv_sem=gs_recv.at[owner],
            device_id=(k ^ m, d), device_id_type=MESH)

    for m in range(1, ns):
        grad_copy(m, k).start()

    def table_copy(m, c, owner):
        e = d ^ m
        return pltpu.make_async_remote_copy(
            src_ref=xt.at[pl.ds(pl.multiple_of(e * cols, cols), cols), pl.ds(c * ch, ch)],
            dst_ref=tb.at[:, pl.ds(pl.multiple_of(owner * rows + c * ch, ch), ch)],
            send_sem=t_send.at[m, c], recv_sem=t_recv.at[owner, c],
            device_id=(k, e), device_id_type=MESH)

    own_half = d // per
    near = list(range(per - 1, 1, -1))
    far = list(range(nc - 1, per - 1, -1))

    def turn(half, c):
        at = pl.ds(pl.multiple_of(half * LANES, LANES), LANES)
        xt[at, pl.ds(c * ch, ch)] = x[pl.ds(c * ch, ch), at].T

    queue = []
    for c in range(CHUNKS):
        loads[c].wait()
        turn(own_half, c)
        for m in queue:
            table_copy(m, c - 1, d).start()
        queue = near
    for c in range(CHUNKS):
        for h in range(1, width // LANES):
            turn(own_half ^ h, c)
        if c == 0:
            for m in near:
                table_copy(m, CHUNKS - 1, d).start()
        else:
            for m in far:
                table_copy(m, c - 1, d).start()

    t = slot_table[k]
    row = ids[pl.ds(t, 1), :]
    low = jnp.bitwise_and(row, LOW - 1).astype(jnp.float32)
    lane = lax.broadcasted_iota(jnp.int32, (LANES, LANES), 1).astype(jnp.float32)
    for b in range(upd // LANES):
        column = jnp.broadcast_to(low[:, b * LANES:(b + 1) * LANES], (LANES, LANES)).T
        for w in range(LOW // LANES):
            onehot[b * LANES:(b + 1) * LANES, w * LANES:(w + 1) * LANES] = jnp.where(
                column == lane + float(w * LANES), 1.0, 0.0).astype(jnp.bfloat16)
    for m in far:
        table_copy(m, CHUNKS - 1, d).start()
    for c in range(CHUNKS):
        table_copy(1, c, d).start()
    high = (row // LOW).astype(jnp.float32)
    hib[...] = jnp.broadcast_to(high, hib.shape).astype(jnp.bfloat16)

    own_grad.wait()
    for m in range(1, ns):
        grad_copy(m, k ^ m).wait_recv()
    g = gbuf[t]
    first = g.astype(jnp.bfloat16)
    rest = g - first.astype(jnp.float32)
    second = rest.astype(jnp.bfloat16)
    third = (rest - second.astype(jnp.float32)).astype(jnp.bfloat16)
    parts[0:cols, :] = first
    parts[cols:2 * cols, :] = second
    parts[2 * cols:3 * cols, :] = third

    def block(step, carry):
        pieces = []
        for i in range(GROUP):
            value = (step * GROUP + i).astype(jnp.float32).astype(jnp.bfloat16)
            pieces.append(jnp.where(hib[...] == value, parts[...], jnp.bfloat16(0)))
        product = jnp.dot(jnp.concatenate(pieces, axis=0), onehot[...],
                          preferred_element_type=jnp.float32)
        for i in range(GROUP):
            base = i * 3 * cols
            piece = (product[base:base + cols] + product[base + cols:base + 2 * cols]) + product[base + 2 * cols:base + 3 * cols]
            at = pl.ds(pl.multiple_of((step * GROUP + i) * LOW, LOW), LOW)
            summed[:, at] = piece
            sq[:, at] = jnp.sum(piece * piece, axis=0, keepdims=True)
        return carry

    lax.fori_loop(0, total_rows // (LOW * GROUP), block, 0)

    def span_of(e):
        return pl.ds(pl.multiple_of(e * rows, rows), rows)

    def sq_copy(m, owner):
        return pltpu.make_async_remote_copy(
            src_ref=sq.at[:, span_of(d ^ m)], dst_ref=rs.at[owner],
            send_sem=q_send.at[m], recv_sem=q_recv.at[owner],
            device_id=(k, d ^ m), device_id_type=MESH)

    for m in range(nc - 1, 0, -1):
        sq_copy(m, d).start()
    tb[:, span_of(d)] = xt[pl.ds(pl.multiple_of(d * cols, cols), cols), :]
    total = sq[:, span_of(d)]
    for m in range(1, nc):
        sq_copy(m, d ^ m).wait_recv()
        total = total + rs[d ^ m]
    stbuf[:, span_of(d)] = state[...] + total / width

    def state_copy(m, owner):
        return pltpu.make_async_remote_copy(
            src_ref=stbuf.at[:, span_of(d)], dst_ref=stbuf.at[:, span_of(owner)],
            send_sem=s_send.at[m], recv_sem=s_recv.at[owner],
            device_id=(k, d ^ m), device_id_type=MESH)

    for m in range(nc - 1, 0, -1):
        state_copy(m, d).start()

    def finish(m):
        e = d ^ m
        at = span_of(e)
        if m:
            state_copy(m, e).wait_recv()
        scale = learn_rate / (jnp.sqrt(stbuf[:, at]) + epsilon)
        if m:
            for c in range(CHUNKS):
                table_copy(m, c, e).wait_recv()
        summed[:, at] = tb[:, at] - summed[:, at] * scale
        pltpu.make_async_copy(summed.at[:, at], out.at[0, :, at], o_sem.at[m]).start()

    order = [0, 1] + near + far[::-1]
    for m in order:
        finish(m)
    state_out[...] = stbuf[...]
    for m in range(1, ns):
        grad_copy(m, k).wait_send()
    for m in range(1, nc):
        for c in range(CHUNKS):
            table_copy(m, c, d).wait_send()
        sq_copy(m, d).wait_send()
        state_copy(m, d).wait_send()
    for m in order:
        at = span_of(d ^ m)
        pltpu.make_async_copy(summed.at[:, at], out.at[0, :, at], o_sem.at[m]).wait()


def solution(mesh):
    ns, nc = mesh.shape["src"], mesh.shape["col"]

    def body(saved_tables, saved_state, slot_table, row_ids, grads):
        _, rows, width = saved_tables.shape
        _, cols, upd = grads.shape
        total_rows = rows * nc
        f32, bf16 = jnp.float32, jnp.bfloat16
        vmem = pl.BlockSpec(memory_space=pltpu.VMEM)
        hbm = pl.BlockSpec(memory_space=pl.ANY)
        dma = pltpu.SemaphoreType.DMA
        return pl.pallas_call(
            functools.partial(kernel, ns, nc),
            out_shape=(jax.ShapeDtypeStruct((1, cols, total_rows), f32),
                       jax.ShapeDtypeStruct((1, total_rows), f32)),
            in_specs=[hbm, vmem, pl.BlockSpec(memory_space=pltpu.SMEM), vmem, hbm],
            out_specs=(hbm, vmem),
            scratch_shapes=[
                pltpu.VMEM((rows, width), f32),
                pltpu.VMEM((width, rows), f32),
                pltpu.VMEM((cols, total_rows), f32),
                pltpu.VMEM((cols, total_rows), f32),
                pltpu.VMEM((ns, cols, upd), f32),
                pltpu.VMEM((3 * cols, upd), bf16),
                pltpu.VMEM((3 * cols, upd), bf16),
                pltpu.VMEM((upd, LOW), bf16),
                pltpu.VMEM((1, total_rows), f32),
                pltpu.VMEM((nc, 1, rows), f32),
                pltpu.VMEM((1, total_rows), f32),
                dma((CHUNKS,)), dma(()), dma((ns,)), dma((ns,)),
                dma((nc, CHUNKS)), dma((nc, CHUNKS)),
                dma((nc,)), dma((nc,)), dma((nc,)), dma((nc,)), dma((nc,)),
            ],
            compiler_params=pltpu.CompilerParams(collective_id=0, has_side_effects=True),
        )(saved_tables, saved_state, slot_table, row_ids, grads)

    return jax.shard_map(
        body,
        mesh=mesh,
        in_specs=(P("src", "col", None), P("src", "col"), P(), P(), P("src", "col", None)),
        out_specs=(P("src", "col", None), P("src", None)),
        check_vma=False,
    )
```

```python
import functools

import jax
import jax.numpy as jnp
from jax import lax
from jax.experimental import pallas as pl
from jax.experimental.pallas import tpu as pltpu
from jax.sharding import PartitionSpec as P

learn_rate = 0.5
epsilon = 1e-08

MESH = pl.DeviceIdType.MESH
LANES = 128
LOW = 256
GROUP = 4
VMEM_LIMIT = 50 << 20
CHUNKS = 4
EARLY = 2
MIDDLE = 1


def kernel(ns, nc, tab, state, slot_table, ids, grads, out, state_out,
           x, xt, tb, summed, gbuf, parts, hib, onehot, sq, rs, stbuf,
           x_sem, g_sem, gs_send, gs_recv, t_send, t_recv,
           q_send, q_recv, s_send, s_recv):
    k = lax.axis_index("src")
    d = lax.axis_index("col")
    rows, width = x.shape
    cols, upd = gbuf.shape[1], gbuf.shape[2]
    total_rows = tb.shape[1]
    per = LANES // cols
    ch = rows // CHUNKS

    loads = []
    for c in range(CHUNKS):
        span = pl.ds(c * ch, ch)
        load = pltpu.make_async_copy(tab.at[0, span], x.at[span], x_sem.at[c])
        load.start()
        loads.append(load)
    own_grad = pltpu.make_async_copy(grads.at[0], gbuf.at[k], g_sem)
    own_grad.start()

    barrier = pltpu.get_barrier_semaphore()
    for m in range(1, nc):
        pl.semaphore_signal(barrier, inc=1, device_id=(k, d ^ m), device_id_type=MESH)
    for m in range(1, ns):
        pl.semaphore_signal(barrier, inc=1, device_id=(k ^ m, d), device_id_type=MESH)

    def grad_copy(m, owner):
        return pltpu.make_async_remote_copy(
            src_ref=grads.at[0], dst_ref=gbuf.at[owner],
            send_sem=gs_send.at[m], recv_sem=gs_recv.at[owner],
            device_id=(k ^ m, d), device_id_type=MESH)


    def table_copy(m, c, owner):
        e = d ^ m
        return pltpu.make_async_remote_copy(
            src_ref=xt.at[pl.ds(pl.multiple_of(e * cols, cols), cols), pl.ds(c * ch, ch)],
            dst_ref=tb.at[:, pl.ds(pl.multiple_of(owner * rows + c * ch, ch), ch)],
            send_sem=t_send.at[m, c], recv_sem=t_recv.at[owner, c],
            device_id=(k, e), device_id_type=MESH)

    own_half = d // per
    near = list(range(per - 1, 1, -1))
    far = list(range(per, nc))

    def turn(half, c):
        at = pl.ds(pl.multiple_of(half * LANES, LANES), LANES)
        xt[at, pl.ds(c * ch, ch)] = x[pl.ds(c * ch, ch), at].T

    for c in range(CHUNKS):
        loads[c].wait()
        for h in range(1, width // LANES):
            turn(own_half ^ h, c)
    pl.semaphore_wait(barrier, nc + ns - 2)
    for c in range(EARLY):
        for m in far:
            table_copy(m, c, d).start()
    for m in range(1, ns):
        grad_copy(m, k).start()
    for c in range(CHUNKS):
        turn(own_half, c)
        if c:
            for m in near:
                table_copy(m, c - 1, d).start()

    t = slot_table[k]
    row = ids[pl.ds(t, 1), :]
    low = jnp.bitwise_and(row, LOW - 1).astype(jnp.float32)
    lane = lax.broadcasted_iota(jnp.int32, (LANES, LANES), 1).astype(jnp.float32)
    for b in range(upd // LANES):
        column = jnp.broadcast_to(low[:, b * LANES:(b + 1) * LANES], (LANES, LANES)).T
        for w in range(LOW // LANES):
            onehot[b * LANES:(b + 1) * LANES, w * LANES:(w + 1) * LANES] = jnp.where(
                column == lane + float(w * LANES), 1.0, 0.0).astype(jnp.bfloat16)
    for m in near:
        table_copy(m, CHUNKS - 1, d).start()
    for c in range(CHUNKS):
        table_copy(1, c, d).start()
    high = (row // LOW).astype(jnp.float32)
    hib[...] = jnp.broadcast_to(high, hib.shape).astype(jnp.bfloat16)

    own_grad.wait()
    for m in range(1, ns):
        grad_copy(m, k ^ m).wait_recv()
    g = gbuf[t]
    first = g.astype(jnp.bfloat16)
    rest = g - first.astype(jnp.float32)
    second = rest.astype(jnp.bfloat16)
    third = (rest - second.astype(jnp.float32)).astype(jnp.bfloat16)
    parts[0:cols, :] = first
    parts[cols:2 * cols, :] = second
    parts[2 * cols:3 * cols, :] = third

    def block(step, carry):
        pieces = []
        for i in range(GROUP):
            value = (step * GROUP + i).astype(jnp.float32).astype(jnp.bfloat16)
            pieces.append(jnp.where(hib[...] == value, parts[...], jnp.bfloat16(0)))
        product = jnp.dot(jnp.concatenate(pieces, axis=0), onehot[...],
                          preferred_element_type=jnp.float32)
        for i in range(GROUP):
            base = i * 3 * cols
            piece = (product[base:base + cols] + product[base + cols:base + 2 * cols]) + product[base + 2 * cols:base + 3 * cols]
            at = pl.ds(pl.multiple_of((step * GROUP + i) * LOW, LOW), LOW)
            summed[:, at] = piece
            sq[:, at] = jnp.sum(piece * piece, axis=0, keepdims=True)
        return carry

    lax.fori_loop(0, total_rows // (LOW * GROUP), block, 0)

    def span_of(e):
        return pl.ds(pl.multiple_of(e * rows, rows), rows)

    def sq_copy(m, owner):
        return pltpu.make_async_remote_copy(
            src_ref=sq.at[:, span_of(d ^ m)], dst_ref=rs.at[owner],
            send_sem=q_send.at[m], recv_sem=q_recv.at[owner],
            device_id=(k, d ^ m), device_id_type=MESH)

    for m in range(nc - 1, 0, -1):
        sq_copy(m, d).start()
    for c in range(EARLY, EARLY + MIDDLE):
        for m in far:
            table_copy(m, c, d).start()
    tb[:, span_of(d)] = xt[pl.ds(pl.multiple_of(d * cols, cols), cols), :]
    total = sq[:, span_of(d)]
    for m in range(1, nc):
        sq_copy(m, d ^ m).wait_recv()
        total = total + rs[d ^ m]
    stbuf[:, span_of(d)] = state[...] + total / width

    def state_copy(m, owner):
        return pltpu.make_async_remote_copy(
            src_ref=stbuf.at[:, span_of(d)], dst_ref=stbuf.at[:, span_of(owner)],
            send_sem=s_send.at[m], recv_sem=s_recv.at[owner],
            device_id=(k, d ^ m), device_id_type=MESH)

    for m in range(nc - 1, 0, -1):
        state_copy(m, d).start()
    for c in range(EARLY + MIDDLE, CHUNKS):
        for m in far:
            table_copy(m, c, d).start()

    def finish(m):
        e = d ^ m
        at = span_of(e)
        if m:
            state_copy(m, e).wait_recv()
        scale = learn_rate / (jnp.sqrt(stbuf[:, at]) + epsilon)
        if m:
            for c in range(CHUNKS):
                table_copy(m, c, e).wait_recv()
        out[0, :, at] = tb[:, at] - summed[:, at] * scale

    order = [0, 1] + near + far
    for m in order:
        finish(m)
    state_out[...] = stbuf[...]
    for m in range(1, ns):
        grad_copy(m, k).wait_send()
    for m in range(1, nc):
        for c in range(CHUNKS):
            table_copy(m, c, d).wait_send()
        sq_copy(m, d).wait_send()
        state_copy(m, d).wait_send()


def solution(mesh):
    ns, nc = mesh.shape["src"], mesh.shape["col"]

    def body(saved_tables, saved_state, slot_table, row_ids, grads):
        _, rows, width = saved_tables.shape
        _, cols, upd = grads.shape
        total_rows = rows * nc
        f32, bf16 = jnp.float32, jnp.bfloat16
        vmem = pl.BlockSpec(memory_space=pltpu.VMEM)
        hbm = pl.BlockSpec(memory_space=pl.ANY)
        dma = pltpu.SemaphoreType.DMA
        return pl.pallas_call(
            functools.partial(kernel, ns, nc),
            out_shape=(jax.ShapeDtypeStruct((1, cols, total_rows), f32),
                       jax.ShapeDtypeStruct((1, total_rows), f32)),
            in_specs=[hbm, vmem, pl.BlockSpec(memory_space=pltpu.SMEM), vmem, hbm],
            out_specs=(vmem, vmem),
            scratch_shapes=[
                pltpu.VMEM((rows, width), f32),
                pltpu.VMEM((width, rows), f32),
                pltpu.VMEM((cols, total_rows), f32),
                pltpu.VMEM((cols, total_rows), f32),
                pltpu.VMEM((ns, cols, upd), f32),
                pltpu.VMEM((3 * cols, upd), bf16),
                pltpu.VMEM((3 * cols, upd), bf16),
                pltpu.VMEM((upd, LOW), bf16),
                pltpu.VMEM((1, total_rows), f32),
                pltpu.VMEM((nc, 1, rows), f32),
                pltpu.VMEM((1, total_rows), f32),
                dma((CHUNKS,)), dma(()), dma((ns,)), dma((ns,)),
                dma((nc, CHUNKS)), dma((nc, CHUNKS)),
                dma((nc,)), dma((nc,)), dma((nc,)), dma((nc,)),
            ],
            compiler_params=pltpu.CompilerParams(collective_id=0, vmem_limit_bytes=VMEM_LIMIT, has_side_effects=True),
        )(saved_tables, saved_state, slot_table, row_ids, grads)

    return jax.shard_map(
        body,
        mesh=mesh,
        in_specs=(P("src", "col", None), P("src", "col"), P(), P(), P("src", "col", None)),
        out_specs=(P("src", "col", None), P("src", None)),
        check_vma=False,
    )
```

```python
import functools

import jax
import jax.numpy as jnp
from jax import lax
from jax.experimental import pallas as pl
from jax.experimental.pallas import tpu as pltpu
from jax.sharding import PartitionSpec as P

learn_rate = 0.5
epsilon = 1e-08

MESH = pl.DeviceIdType.MESH
LANES = 128
LOW = 256
GROUP = 8
VMEM_LIMIT = 50 << 20
CHUNKS = 4
EARLY = 2
MIDDLE = 1


def kernel(ns, nc, tab, state, slot_table, ids, grads, out, state_out,
           x, xt, tb, summed, gbuf, parts, hib, onehot, sq, rs, stbuf,
           x_sem, g_sem, gs_send, gs_recv, t_send, t_recv,
           q_send, q_recv, s_send, s_recv):
    k = lax.axis_index("src")
    d = lax.axis_index("col")
    rows, width = x.shape
    cols, upd = gbuf.shape[1], gbuf.shape[2]
    total_rows = tb.shape[1]
    per = LANES // cols
    ch = rows // CHUNKS

    loads = []
    for c in range(CHUNKS):
        span = pl.ds(c * ch, ch)
        load = pltpu.make_async_copy(tab.at[0, span], x.at[span], x_sem.at[c])
        load.start()
        loads.append(load)
    own_grad = pltpu.make_async_copy(grads.at[0], gbuf.at[k], g_sem)
    own_grad.start()

    barrier = pltpu.get_barrier_semaphore()
    for m in range(1, nc):
        pl.semaphore_signal(barrier, inc=1, device_id=(k, d ^ m), device_id_type=MESH)
    for m in range(1, ns):
        pl.semaphore_signal(barrier, inc=1, device_id=(k ^ m, d), device_id_type=MESH)

    def grad_copy(m, owner):
        return pltpu.make_async_remote_copy(
            src_ref=grads.at[0], dst_ref=gbuf.at[owner],
            send_sem=gs_send.at[m], recv_sem=gs_recv.at[owner],
            device_id=(k ^ m, d), device_id_type=MESH)


    def table_copy(m, c, owner):
        e = d ^ m
        return pltpu.make_async_remote_copy(
            src_ref=xt.at[pl.ds(pl.multiple_of(e * cols, cols), cols), pl.ds(c * ch, ch)],
            dst_ref=tb.at[:, pl.ds(pl.multiple_of(owner * rows + c * ch, ch), ch)],
            send_sem=t_send.at[m, c], recv_sem=t_recv.at[owner, c],
            device_id=(k, e), device_id_type=MESH)

    own_half = d // per
    near = list(range(per - 1, 1, -1))
    far = list(range(per, nc))

    def turn(half, c):
        at = pl.ds(pl.multiple_of(half * LANES, LANES), LANES)
        xt[at, pl.ds(c * ch, ch)] = x[pl.ds(c * ch, ch), at].T

    for c in range(CHUNKS):
        loads[c].wait()
        for h in range(1, width // LANES):
            turn(own_half ^ h, c)
    pl.semaphore_wait(barrier, nc + ns - 2)
    for c in range(EARLY):
        for m in far:
            table_copy(m, c, d).start()
    for m in range(1, ns):
        grad_copy(m, k).start()
    for c in range(CHUNKS):
        turn(own_half, c)
        if c:
            for m in near:
                table_copy(m, c - 1, d).start()

    t = slot_table[k]
    row = ids[pl.ds(t, 1), :]
    low = jnp.bitwise_and(row, LOW - 1).astype(jnp.float32)
    lane = lax.broadcasted_iota(jnp.int32, (LANES, LANES), 1).astype(jnp.float32)
    for b in range(upd // LANES):
        column = jnp.broadcast_to(low[:, b * LANES:(b + 1) * LANES], (LANES, LANES)).T
        for w in range(LOW // LANES):
            onehot[b * LANES:(b + 1) * LANES, w * LANES:(w + 1) * LANES] = jnp.where(
                column == lane + float(w * LANES), 1.0, 0.0).astype(jnp.bfloat16)
    for m in near:
        table_copy(m, CHUNKS - 1, d).start()
    for c in range(CHUNKS):
        table_copy(1, c, d).start()
    high = (row // LOW).astype(jnp.float32)
    hib[...] = jnp.broadcast_to(high, hib.shape).astype(jnp.bfloat16)

    own_grad.wait()
    for m in range(1, ns):
        grad_copy(m, k ^ m).wait_recv()
    g = gbuf[t]
    first = g.astype(jnp.bfloat16)
    rest = g - first.astype(jnp.float32)
    second = rest.astype(jnp.bfloat16)
    third = (rest - second.astype(jnp.float32)).astype(jnp.bfloat16)
    parts[0:cols, :] = first
    parts[cols:2 * cols, :] = second
    parts[2 * cols:3 * cols, :] = third

    def block(step, carry):
        pieces = []
        for i in range(GROUP):
            value = (step * GROUP + i).astype(jnp.float32).astype(jnp.bfloat16)
            pieces.append(jnp.where(hib[...] == value, parts[...], jnp.bfloat16(0)))
        product = jnp.dot(jnp.concatenate(pieces, axis=0), onehot[...],
                          preferred_element_type=jnp.float32)
        for i in range(GROUP):
            base = i * 3 * cols
            piece = (product[base:base + cols] + product[base + cols:base + 2 * cols]) + product[base + 2 * cols:base + 3 * cols]
            at = pl.ds(pl.multiple_of((step * GROUP + i) * LOW, LOW), LOW)
            summed[:, at] = piece
            sq[:, at] = jnp.sum(piece * piece, axis=0, keepdims=True)
        return carry


    def span_of(e):
        return pl.ds(pl.multiple_of(e * rows, rows), rows)

    def sq_copy(m, owner):
        return pltpu.make_async_remote_copy(
            src_ref=sq.at[:, span_of(d ^ m)], dst_ref=rs.at[owner],
            send_sem=q_send.at[m], recv_sem=q_recv.at[owner],
            device_id=(k, d ^ m), device_id_type=MESH)

    steps = rows // (LOW * GROUP)
    ready = None
    for m in far + near + [1, 0]:
        base = (d ^ m) * steps
        lax.fori_loop(base, base + steps, block, 0)
        if ready is not None:
            sq_copy(ready, d).start()
        ready = m
    for c in range(EARLY, EARLY + MIDDLE):
        for m in far:
            table_copy(m, c, d).start()
    tb[:, span_of(d)] = xt[pl.ds(pl.multiple_of(d * cols, cols), cols), :]
    total = sq[:, span_of(d)]
    for m in range(1, nc):
        sq_copy(m, d ^ m).wait_recv()
        total = total + rs[d ^ m]
    stbuf[:, span_of(d)] = state[...] + total / width

    def state_copy(m, owner):
        return pltpu.make_async_remote_copy(
            src_ref=stbuf.at[:, span_of(d)], dst_ref=stbuf.at[:, span_of(owner)],
            send_sem=s_send.at[m], recv_sem=s_recv.at[owner],
            device_id=(k, d ^ m), device_id_type=MESH)

    for m in range(nc - 1, 0, -1):
        state_copy(m, d).start()
    for c in range(EARLY + MIDDLE, CHUNKS):
        for m in far:
            table_copy(m, c, d).start()

    def finish(m):
        e = d ^ m
        at = span_of(e)
        if m:
            state_copy(m, e).wait_recv()
        scale = learn_rate / (jnp.sqrt(stbuf[:, at]) + epsilon)
        if m:
            for c in range(CHUNKS):
                table_copy(m, c, e).wait_recv()
        out[0, :, at] = tb[:, at] - summed[:, at] * scale

    order = [0, 1] + near + far
    for m in order:
        finish(m)
    state_out[...] = stbuf[...]
    for m in range(1, ns):
        grad_copy(m, k).wait_send()
    for m in range(1, nc):
        for c in range(CHUNKS):
            table_copy(m, c, d).wait_send()
        sq_copy(m, d).wait_send()
        state_copy(m, d).wait_send()


def solution(mesh):
    ns, nc = mesh.shape["src"], mesh.shape["col"]

    def body(saved_tables, saved_state, slot_table, row_ids, grads):
        _, rows, width = saved_tables.shape
        _, cols, upd = grads.shape
        total_rows = rows * nc
        f32, bf16 = jnp.float32, jnp.bfloat16
        vmem = pl.BlockSpec(memory_space=pltpu.VMEM)
        hbm = pl.BlockSpec(memory_space=pl.ANY)
        dma = pltpu.SemaphoreType.DMA
        return pl.pallas_call(
            functools.partial(kernel, ns, nc),
            out_shape=(jax.ShapeDtypeStruct((1, cols, total_rows), f32),
                       jax.ShapeDtypeStruct((1, total_rows), f32)),
            in_specs=[hbm, vmem, pl.BlockSpec(memory_space=pltpu.SMEM), vmem, hbm],
            out_specs=(vmem, vmem),
            scratch_shapes=[
                pltpu.VMEM((rows, width), f32),
                pltpu.VMEM((width, rows), f32),
                pltpu.VMEM((cols, total_rows), f32),
                pltpu.VMEM((cols, total_rows), f32),
                pltpu.VMEM((ns, cols, upd), f32),
                pltpu.VMEM((3 * cols, upd), bf16),
                pltpu.VMEM((3 * cols, upd), bf16),
                pltpu.VMEM((upd, LOW), bf16),
                pltpu.VMEM((1, total_rows), f32),
                pltpu.VMEM((nc, 1, rows), f32),
                pltpu.VMEM((1, total_rows), f32),
                dma((CHUNKS,)), dma(()), dma((ns,)), dma((ns,)),
                dma((nc, CHUNKS)), dma((nc, CHUNKS)),
                dma((nc,)), dma((nc,)), dma((nc,)), dma((nc,)),
            ],
            compiler_params=pltpu.CompilerParams(collective_id=0, vmem_limit_bytes=VMEM_LIMIT, has_side_effects=True),
        )(saved_tables, saved_state, slot_table, row_ids, grads)

    return jax.shard_map(
        body,
        mesh=mesh,
        in_specs=(P("src", "col", None), P("src", "col"), P(), P(), P("src", "col", None)),
        out_specs=(P("src", "col", None), P("src", None)),
        check_vma=False,
    )
```
